32 devices in a mesh: dp: 8 (over z, x), mp: 4 (over y, core).
Axes of the slice: x: 2, y: 2, z: 4, core: 2. Of those that a mesh axis runs over, the one named last changes fastest.
Arguments:
- gradients: bfloat16 [8, 3584, 14336], P(None, 'dp', 'mp'), may hold values from -60 to 60
- column_slot: int32 [8, 16], replicated, may hold values from 0 to 31, as said below
- left_roots: bfloat16 [32, 4, 4, 896, 896], P('dp', 'mp'), may hold values from -1 to 5
- right_roots: bfloat16 [32, 4, 4, 896, 896], P('dp', 'mp'), may hold values from -1 to 5
Outputs:
- update: bfloat16 [8, 3584, 14336], P(None, 'dp', 'mp')
- clip_scale: float32 [], replicated
The draws below stay inside these ranges and needn't reach their ends.
Inputs may be any that keep to these rules, and one draw needn't show every extreme that they name: `column_slot`: block column c belongs to group c // 4; over all matrices, the entries of one group's block columns are a permutation of 0 to 31.
All inputs are finite; a program needn't handle non-finite values.
Results may differ from the reference program's by a relative error of at most 0.0049.
Values may be sent and summed in bfloat16 or wider, within the bound.
A program may use at most 256 MiB of HBM per device.

```python
import math
import jax
import jax.numpy as jnp
from jax import lax

D = 3584
FF = 14336
BLOCK = 896
MATRICES = 8
ROW_BLOCKS = 4
COLUMNS = 16
COLS_MP = 4
SLOTS = 32
N_MP = 4


def draw_gradients(key, part):
    keys = jax.random.split(jax.random.fold_in(key, 5), 3)
    ramp = jnp.sqrt(1.0 + 2.0 * jnp.arange(D, dtype=jnp.float32) / (D - 1)).reshape(1, D, 1)
    col_scale = jnp.exp(jax.random.uniform(keys[1], (MATRICES, 1, FF), jnp.float32, 0.0, math.log(10.0)))
    row_scale = jnp.exp(jax.random.uniform(keys[0], (MATRICES, D, 1), jnp.float32, 0.0, math.log(10.0)))
    base = jnp.clip(jax.random.normal(keys[2], (MATRICES, D, FF), jnp.float32), -6.0, 6.0)
    values = base * row_scale * col_scale * ramp / 21.5
    return jnp.clip(values, -60.0, 60.0).astype(jnp.bfloat16)


def draw_column_slot(key, part):
    keys = jax.random.split(jax.random.fold_in(key, 11), N_MP)

    def permute_one(sub_key):
        return jax.random.permutation(sub_key, SLOTS)
    perms = jax.vmap(permute_one)(keys).astype(jnp.int32)
    table = perms.reshape(N_MP, MATRICES, COLS_MP).transpose(1, 0, 2).reshape(MATRICES, COLUMNS)
    return table.astype(jnp.int32)


def draw_roots(key):
    keys = jax.random.split(key, 2)
    shape = (SLOTS, N_MP, ROW_BLOCKS, BLOCK, BLOCK)
    noise = jnp.clip(jax.random.normal(keys[0], shape, jnp.float32), -4.0, 4.0)
    symmetric = (noise + jnp.swapaxes(noise, -1, -2)) * (0.35 / math.sqrt(2.0 * BLOCK))
    diagonal = jnp.exp(jax.random.uniform(keys[1], shape[:-1], jnp.float32, math.log(0.5), math.log(2.0)))
    matrix = symmetric + diagonal[..., None] * jnp.eye(BLOCK, dtype=jnp.float32)
    return matrix.astype(jnp.bfloat16)


def draw_left_roots(key, part):
    return draw_roots(jax.random.fold_in(key, 21))


def draw_right_roots(key, part):
    return draw_roots(jax.random.fold_in(key, 37))


def setup_inputs(seed: int = 0) -> dict:
    splits = jax.random.split(jax.random.key(seed), 5)
    gradients = draw_gradients(jax.random.fold_in(splits[4], 71), 0)
    column_slot = draw_column_slot(jax.random.fold_in(splits[4], 71), 0)
    left_roots = draw_left_roots(jax.random.fold_in(splits[4], 71), 0)
    right_roots = draw_right_roots(jax.random.fold_in(splits[4], 71), 0)
    return {"gradients": gradients, "column_slot": column_slot, "left_roots": left_roots, "right_roots": right_roots}


rms_limit = 0.25
epsilon = 1e-06

def reference(gradients, column_slot, left_roots, right_roots):
    widened = gradients.astype(jnp.float32)
    square_sum = jnp.sum(widened * widened)
    mean_square = square_sum / (MATRICES * D * FF)
    clip_scale = jnp.minimum(jnp.float32(1.0), rms_limit / jnp.sqrt(mean_square + epsilon)).astype(jnp.float32)
    zero_index = jnp.zeros((), jnp.int32)

    def one_column(flat_index):
        matrix = (flat_index // COLUMNS).astype(jnp.int32)
        block_col = (flat_index % COLUMNS).astype(jnp.int32)
        group_index = (block_col // COLS_MP).astype(jnp.int32)
        slot_index = column_slot[matrix, block_col].astype(jnp.int32)
        block_grad = lax.dynamic_slice(gradients, (matrix, zero_index, (block_col * BLOCK).astype(jnp.int32)), (1, D, BLOCK))
        block_grad = block_grad.reshape(ROW_BLOCKS, BLOCK, BLOCK).astype(jnp.float32)
        starts = (slot_index, group_index, zero_index, zero_index, zero_index)
        left_root = lax.dynamic_slice(left_roots, starts, (1, 1, ROW_BLOCKS, BLOCK, BLOCK)).reshape(ROW_BLOCKS, BLOCK, BLOCK)
        right_root = lax.dynamic_slice(right_roots, starts, (1, 1, ROW_BLOCKS, BLOCK, BLOCK)).reshape(ROW_BLOCKS, BLOCK, BLOCK)
        first_product = jnp.einsum('nab,nbc->nac', left_root.astype(jnp.float32), block_grad)
        scaled = (clip_scale * first_product).astype(jnp.bfloat16)
        second_product = jnp.einsum('nab,nbc->nac', scaled.astype(jnp.float32), right_root.astype(jnp.float32))
        return second_product.astype(jnp.bfloat16).reshape(D, BLOCK)
    columns = lax.map(one_column, jnp.arange(MATRICES * COLUMNS, dtype=jnp.int32))
    update = columns.reshape(MATRICES, COLUMNS, D, BLOCK).transpose(0, 2, 1, 3).reshape(MATRICES, D, FF)
    return (update, clip_scale)
```

```python
import functools
import math

import jax
import jax.numpy as jnp
from jax import lax
from jax.experimental import pallas as pl
from jax.experimental.pallas import tpu as pltpu
from jax.sharding import PartitionSpec as P

rms_limit = 0.25
epsilon = 1e-06
MESH = pl.DeviceIdType.MESH
MIB = 1024 * 1024
LANES = 128
RING = 8


def partner(a, b, n):
    if n & (n - 1):
        return (a + b) % n
    total, bit = 0, 1
    while bit < n:
        total = total + ((a // bit + b // bit) % 2) * bit
        bit *= 2
    return total


def first_kernel(owned, slot_ref, g_ref, packed_ref, table_ref, buf, in_sem, out_sem):
    matrices, rows, width = g_ref.shape
    block = packed_ref.shape[-1]
    peers = packed_ref.shape[0]
    cols = width // block
    base = lax.axis_index("mp") * cols
    for m in range(matrices):
        for c in range(cols):
            s = slot_ref[m, base + c]
            table_ref[s] = m * cols + c

    def read(q):
        m, c = table_ref[q * owned] // cols, table_ref[q * owned] % cols
        src = g_ref.at[m, :, pl.ds(pl.multiple_of(c * block, LANES), block)]
        return pltpu.make_async_copy(src, buf.at[q], in_sem.at[q])

    def write(q):
        return pltpu.make_async_copy(buf.at[q], packed_ref.at[q, 0], out_sem.at[q])

    for q in range(peers):
        read(q).start()
    for q in range(peers):
        read(q).wait()
        write(q).start()
    for q in range(peers):
        write(q).wait()


def first_pack(column_slot, gradients, peers, owned, block):
    rows = gradients.shape[1]
    half = peers * rows * block
    return pl.pallas_call(
        functools.partial(first_kernel, owned),
        in_specs=[
            pl.BlockSpec(memory_space=pltpu.SMEM),
            pl.BlockSpec(memory_space=pltpu.HBM),
        ],
        out_specs=[
            pl.BlockSpec(memory_space=pltpu.HBM),
            pl.BlockSpec(memory_space=pltpu.SMEM),
        ],
        out_shape=[
            pltpu.HBM((peers, owned, rows, block), gradients.dtype),
            pltpu.SMEM((peers * owned,), jnp.int32),
        ],
        scratch_shapes=[
            pltpu.VMEM((peers, rows, block), gradients.dtype),
            pltpu.SemaphoreType.DMA((peers,)),
            pltpu.SemaphoreType.DMA((peers,)),
        ],
        compiler_params=pltpu.CompilerParams(vmem_limit_bytes=56 * MIB),
        cost_estimate=pl.CostEstimate(flops=0, bytes_accessed=4 * half, transcendentals=0),
    )(column_slot, gradients)


def main_kernel(
    total,
    n_mp,
    table_ref,
    packed_in,
    g_ref,
    left_ref,
    right_ref,
    packed,
    returned,
    clip_out,
    received,
    results,
    ga,
    gb,
    stage,
    acc,
    part,
    sums_dp,
    sums_mp,
    x_buf,
    l_buf,
    r_buf,
    o_buf,
    g_sem,
    stage_sem,
    block_sem,
    send_f,
    recv_f,
    send_r,
    recv_r,
    send_dp,
    recv_dp,
    send_mp,
    recv_mp,
):
    del packed_in
    peers, owned, rows, block = packed.shape
    matrices, _, width = g_ref.shape
    row_blocks = left_ref.shape[2]
    halves = block // rows
    me, mp = lax.axis_index("dp"), lax.axis_index("mp")
    my_block, my_half = me // halves, me % halves

    def peer(zo, ho):
        return partner(my_block, zo, row_blocks) * halves + partner(my_half, ho, halves)

    barrier = pltpu.get_barrier_semaphore()
    for o in range(1, peers):
        q = (me + o) % peers
        pl.semaphore_signal(barrier, inc=1, device_id=(q, mp), device_id_type=MESH)
    for o in range(1, n_mp):
        q = (mp + o) % n_mp
        pl.semaphore_signal(barrier, inc=1, device_id=(me, q), device_id_type=MESH)
    pl.semaphore_wait(barrier, peers + n_mp - 2)

    def forward(q, j):
        return pltpu.make_async_remote_copy(
            src_ref=packed.at[q, j],
            dst_ref=received.at[me, j],
            send_sem=send_f.at[q, j],
            recv_sem=recv_f.at[me, j],
            device_id=(q, mp),
            device_id_type=MESH,
        )

    def arrival(q, j):
        return pltpu.make_async_remote_copy(
            src_ref=packed.at[q, j],
            dst_ref=received.at[q, j],
            send_sem=send_f.at[q, j],
            recv_sem=recv_f.at[q, j],
            device_id=(q, mp),
            device_id_type=MESH,
        )

    order = [(zo, ho) for zo in range(1, row_blocks) for ho in range(halves)]
    order = order[len(order) // 3 :] + order[: len(order) // 3]
    order = order + [(0, ho) for ho in range(1, halves)]
    for zo, ho in order:
        forward(peer(zo, ho), 0).start()

    chunk = ga.shape[1]
    cols = width // block
    chunks = rows // chunk
    rest = peers * (owned - 1)
    acc[...] = jnp.zeros_like(acc)

    def load(t):
        buf = ga if t % 2 == 0 else gb

        def column(i, _):
            at = pl.multiple_of((i % cols) * block, LANES)
            src = g_ref.at[i // cols, pl.ds(t * chunk, chunk), pl.ds(at, block)]
            pltpu.make_async_copy(src, buf.at[i], g_sem.at[t % 2]).start()
            return 0

        lax.fori_loop(0, matrices * cols, column, 0)

    def loaded(t):
        buf = ga if t % 2 == 0 else gb
        pltpu.make_async_copy(buf, buf, g_sem.at[t % 2]).wait()

    load(0)
    for t in range(chunks):
        g = ga if t % 2 == 0 else gb
        if t + 1 < chunks:
            load(t + 1)
        loaded(t)

        def stored(n, t=t):
            q, j = n // (owned - 1), 1 + n % (owned - 1)
            return pltpu.make_async_copy(
                stage.at[n % RING],
                packed.at[q, j, pl.ds(t * chunk, chunk), :],
                stage_sem.at[n % RING],
            )

        def move(n, _, g=g, stored=stored):
            q, j = n // (owned - 1), 1 + n % (owned - 1)

            @pl.when(n >= RING)
            def _():
                stored(n - RING).wait()

            stage[n % RING] = g[table_ref[q * owned + j]]
            stored(n).start()
            return 0

        def square(n, _, g=g):
            per = chunk // 16
            x = g[n // per, pl.ds(pl.multiple_of((n % per) * 16, 16), 16), :]
            wide = x.astype(jnp.float32)
            wide = wide * wide
            acc[...] += wide[:8] + wide[8:]
            return 0

        if rest:
            lax.fori_loop(0, rest, move, 0)
        lax.fori_loop(0, matrices * cols * (chunk // 16), square, 0)
        for n in range(max(rest - RING, 0), rest):
            stored(n).wait()

    for j in range(1, owned):
        for zo, ho in order:
            forward(peer(zo, ho), j).start()

    tile = acc[:, :LANES]
    for k in range(1, block // LANES):
        tile += acc[:, k * LANES : (k + 1) * LANES]
    part[0] = tile
    sums_dp[me] = tile

    def spread(o, axis_me, n, src, dst, send, recv, device):
        q = (axis_me + o) % n
        return pltpu.make_async_remote_copy(
            src_ref=src,
            dst_ref=dst.at[axis_me],
            send_sem=send.at[o],
            recv_sem=recv.at[axis_me],
            device_id=device(q),
            device_id_type=MESH,
        )

    def landed(o, axis_me, n, src, dst, send, recv, device):
        q = (axis_me + o) % n
        return pltpu.make_async_remote_copy(
            src_ref=src,
            dst_ref=dst.at[q],
            send_sem=send.at[o],
            recv_sem=recv.at[q],
            device_id=device(q),
            device_id_type=MESH,
        )

    dp_args = (me, peers, part.at[0], sums_dp, send_dp, recv_dp, lambda q: (q, mp))
    mp_args = (mp, n_mp, part.at[1], sums_mp, send_mp, recv_mp, lambda q: (me, q))
    for o in range(1, peers):
        spread(o, *dp_args).start()
    for o in range(1, peers):
        landed(o, *dp_args).wait_recv()
    tile = jnp.sum(sums_dp[...], axis=0)
    part[1] = tile
    sums_mp[mp] = tile
    for o in range(1, n_mp):
        spread(o, *mp_args).start()
    for o in range(1, n_mp):
        landed(o, *mp_args).wait_recv()
    tile = jnp.sum(sums_mp[...], axis=0)
    square_sum = jnp.sum(jnp.sum(tile, axis=0, keepdims=True), axis=1, keepdims=True)
    clip = jnp.minimum(1.0, rms_limit / jnp.sqrt(square_sum / total + epsilon))
    clip_out[...] = jnp.broadcast_to(clip, clip_out.shape)
    for o in range(1, peers):
        spread(o, *dp_args).wait_send()
    for o in range(1, n_mp):
        spread(o, *mp_args).wait_send()

    def ret(q, j, r, h):
        return pltpu.make_async_remote_copy(
            src_ref=results.at[j, r, pl.ds(h * rows, rows), :],
            dst_ref=returned.at[me, j],
            send_sem=send_r.at[q, j],
            recv_sem=recv_r.at[me, j],
            device_id=(q, mp),
            device_id_type=MESH,
        )

    def home(q, j):
        return pltpu.make_async_remote_copy(
            src_ref=results.at[j, 0, pl.ds(0, rows), :],
            dst_ref=returned.at[q, j],
            send_sem=send_r.at[q, j],
            recv_sem=recv_r.at[q, j],
            device_id=(q, mp),
            device_id_type=MESH,
        )

    def one_block(n, _):
        j, k = n // row_blocks, n % row_blocks
        r = partner(my_block, (k + 1) % row_blocks, row_blocks)
        left = pltpu.make_async_copy(left_ref.at[j, 0, r], l_buf, block_sem.at[0])
        right = pltpu.make_async_copy(right_ref.at[j, 0, r], r_buf, block_sem.at[1])
        left.start()
        right.start()
        for h in range(halves):
            q = r * halves + h
            dst = x_buf.at[pl.ds(h * rows, rows), :]

            @pl.when(q == me)
            def _(q=q, h=h, dst=dst):
                pltpu.make_async_copy(packed.at[q, j], dst, block_sem.at[2 + h]).start()

            @pl.when(q != me)
            def _(q=q, h=h, dst=dst):
                arrival(q, j).wait_recv()
                pltpu.make_async_copy(received.at[q, j], dst, block_sem.at[2 + h]).start()

        left.wait()
        right.wait()
        for h in range(halves):
            dst = x_buf.at[pl.ds(h * rows, rows), :]
            pltpu.make_async_copy(packed.at[0, 0], dst, block_sem.at[2 + h]).wait()
        first = jnp.dot(l_buf[...], x_buf[...], preferred_element_type=jnp.float32)
        scaled = (clip_out[0:1, 0:1] * first).astype(jnp.bfloat16)
        second = jnp.dot(scaled, r_buf[...], preferred_element_type=jnp.float32)
        o_buf[...] = second.astype(o_buf.dtype)
        out = pltpu.make_async_copy(o_buf, results.at[j, r], block_sem.at[0])
        out.start()
        out.wait()
        for h in range(halves):
            q = r * halves + h

            @pl.when(q == me)
            def _(q=q, h=h):
                src = o_buf.at[pl.ds(h * rows, rows), :]
                returned[me, j] = src[...]

            @pl.when(q != me)
            def _(q=q, h=h):
                ret(q, j, r, h).start()

        return 0

    lax.fori_loop(0, owned * row_blocks, one_block, 0)

    for j in range(owned):
        for zo, ho in order:
            q = peer(zo, ho)
            forward(q, j).wait_send()
            home(q, j).wait_recv()
            home(q, j).wait_send()


def exchange(mesh, total, table, packed, gradients, left_roots, right_roots):
    peers, owned, rows, block = packed.shape
    matrices, _, width = gradients.shape
    row_blocks = left_roots.shape[2]
    n_mp = mesh.shape["mp"]
    chunk = max(c for c in range(16, 129, 16) if rows % c == 0)
    dtype = gradients.dtype
    dma = pltpu.SemaphoreType.DMA
    count = owned * row_blocks
    anywhere = pl.BlockSpec(memory_space=pltpu.HBM)
    in_vmem = pl.BlockSpec(memory_space=pltpu.VMEM)
    outs = pl.pallas_call(
        functools.partial(main_kernel, total, n_mp),
        in_specs=[pl.BlockSpec(memory_space=pltpu.SMEM)] + [anywhere] * 4,
        out_specs=[anywhere, in_vmem, in_vmem, anywhere, anywhere],
        out_shape=[
            jax.ShapeDtypeStruct(packed.shape, dtype),
            pltpu.VMEM((peers, owned, rows, block), dtype),
            jax.ShapeDtypeStruct((8, LANES), jnp.float32),
            jax.ShapeDtypeStruct(packed.shape, dtype),
            jax.ShapeDtypeStruct((owned, row_blocks, block, block), dtype),
        ],
        scratch_shapes=[
            pltpu.VMEM((peers * owned, chunk, block), dtype),
            pltpu.VMEM((peers * owned, chunk, block), dtype),
            pltpu.VMEM((RING, chunk, block), dtype),
            pltpu.VMEM((8, block), jnp.float32),
            pltpu.VMEM((2, 8, LANES), jnp.float32),
            pltpu.VMEM((peers, 8, LANES), jnp.float32),
            pltpu.VMEM((n_mp, 8, LANES), jnp.float32),
            pltpu.VMEM((block, block), dtype),
            pltpu.VMEM((block, block), dtype),
            pltpu.VMEM((block, block), dtype),
            pltpu.VMEM((block, block), dtype),
            dma((2,)),
            dma((RING,)),
            dma((2 + block // rows,)),
            dma((peers, owned)),
            dma((peers, owned)),
            dma((peers, owned)),
            dma((peers, owned)),
            dma((peers,)),
            dma((peers,)),
            dma((n_mp,)),
            dma((n_mp,)),
        ],
        input_output_aliases={1: 0},
        compiler_params=pltpu.CompilerParams(
            collective_id=0, has_side_effects=True, vmem_limit_bytes=36 * MIB
        ),
        cost_estimate=pl.CostEstimate(
            flops=4 * count * block**3,
            bytes_accessed=8 * count * block**2,
            transcendentals=0,
        ),
    )(table, packed, gradients, left_roots, right_roots)
    return outs[1], outs[2]


def last_kernel(owned, table_ref, x_ref, o_ref, sems):
    peers, _, rows, block = x_ref.shape
    cols = o_ref.shape[2] // block

    def put(s):
        m, c = table_ref[s] // cols, table_ref[s] % cols
        dst = o_ref.at[m, :, pl.ds(pl.multiple_of(c * block, LANES), block)]
        return pltpu.make_async_copy(x_ref.at[s // owned, s % owned], dst, sems.at[s])

    for s in range(peers * owned):
        put(s).start()
    for s in range(peers * owned):
        put(s).wait()


def unpack(table, returned, shape):
    peers, owned, rows, block = returned.shape
    return pl.pallas_call(
        functools.partial(last_kernel, owned),
        in_specs=[
            pl.BlockSpec(memory_space=pltpu.SMEM),
            pl.BlockSpec(memory_space=pltpu.VMEM),
        ],
        out_specs=pl.BlockSpec(memory_space=pltpu.HBM),
        out_shape=jax.ShapeDtypeStruct(shape, returned.dtype),
        scratch_shapes=[pltpu.SemaphoreType.DMA((peers * owned,))],
        compiler_params=pltpu.CompilerParams(vmem_limit_bytes=4 * MIB),
        cost_estimate=pl.CostEstimate(
            flops=0, bytes_accessed=2 * math.prod(shape), transcendentals=0
        ),
    )(table, returned)


def body(mesh, total, gradients, column_slot, left_roots, right_roots):
    owned, block = left_roots.shape[0], left_roots.shape[-1]
    peers = mesh.shape["dp"]
    packed, table = first_pack(column_slot, gradients, peers, owned, block)
    returned, clip = exchange(
        mesh, total, table, packed, gradients, left_roots, right_roots
    )
    update = unpack(table, returned, gradients.shape)
    return (update, clip[0, 0])


def solution(mesh):
    def run(gradients, column_slot, left_roots, right_roots):
        mapped = jax.shard_map(
            functools.partial(body, mesh, math.prod(gradients.shape)),
            mesh=mesh,
            in_specs=(
                P(None, "dp", "mp"),
                P(),
                P("dp", "mp", None, None, None),
                P("dp", "mp", None, None, None),
            ),
            out_specs=(P(None, "dp", "mp"), P()),
            check_vma=False,
        )
        return mapped(gradients, column_slot, left_roots, right_roots)

    return run
```

```python
import functools
import math

import jax
import jax.numpy as jnp
from jax import lax
from jax.experimental import pallas as pl
from jax.experimental.pallas import tpu as pltpu
from jax.sharding import PartitionSpec as P

rms_limit = 0.25
epsilon = 1e-06
MESH = pl.DeviceIdType.MESH
MIB = 1024 * 1024
LANES = 128
RING = 8


def partner(a, b, n):
    if n & (n - 1):
        return (a + b) % n
    total, bit = 0, 1
    while bit < n:
        total = total + ((a // bit + b // bit) % 2) * bit
        bit *= 2
    return total


def peer_of(zo, ho, row_blocks, halves):
    me, mp = lax.axis_index("dp"), lax.axis_index("mp")
    block, half = me // halves, me % halves
    if not (isinstance(zo, int) and zo == 0):
        ho = (ho + mp) % halves
    return partner(block, zo, row_blocks) * halves + partner(half, ho, halves)


NEAR = 2


def first_kernel(
    owned, row_blocks, slot_ref, g_ref, packed_ref, table_ref, buf, in_sem, out_sem
):
    matrices, rows, width = g_ref.shape
    block = packed_ref.shape[-1]
    peers = packed_ref.shape[0]
    halves = peers // row_blocks
    first = [
        peer_of(zo, ho, row_blocks, halves)
        for zo in range(NEAR, row_blocks)
        for ho in range(halves)
    ]
    cols = width // block
    base = lax.axis_index("mp") * cols
    for m in range(matrices):
        for c in range(cols):
            s = slot_ref[m, base + c]
            table_ref[s] = m * cols + c

    def read(k):
        s = table_ref[first[k] * owned]
        at = pl.multiple_of((s % cols) * block, LANES)
        src = g_ref.at[s // cols, :, pl.ds(at, block)]
        return pltpu.make_async_copy(src, buf.at[k], in_sem.at[k])

    def write(k):
        return pltpu.make_async_copy(buf.at[k], packed_ref.at[first[k], 0], out_sem.at[k])

    for k in range(len(first)):
        read(k).start()
    for k in range(len(first)):
        read(k).wait()
        write(k).start()
    for k in range(len(first)):
        write(k).wait()


def first_pack(column_slot, gradients, peers, owned, row_blocks, block):
    rows = gradients.shape[1]
    half = peers * rows * block
    return pl.pallas_call(
        functools.partial(first_kernel, owned, row_blocks),
        in_specs=[
            pl.BlockSpec(memory_space=pltpu.SMEM),
            pl.BlockSpec(memory_space=pltpu.HBM),
        ],
        out_specs=[
            pl.BlockSpec(memory_space=pltpu.HBM),
            pl.BlockSpec(memory_space=pltpu.SMEM),
        ],
        out_shape=[
            pltpu.HBM((peers, owned, rows, block), gradients.dtype),
            pltpu.SMEM((peers * owned,), jnp.int32),
        ],
        scratch_shapes=[
            pltpu.VMEM((peers, rows, block), gradients.dtype),
            pltpu.SemaphoreType.DMA((peers,)),
            pltpu.SemaphoreType.DMA((peers,)),
        ],
        compiler_params=pltpu.CompilerParams(vmem_limit_bytes=56 * MIB),
        cost_estimate=pl.CostEstimate(flops=0, bytes_accessed=4 * half, transcendentals=0),
    )(column_slot, gradients)


def main_kernel(
    total,
    n_mp,
    table_ref,
    packed_in,
    g_ref,
    left_ref,
    right_ref,
    packed,
    returned,
    clip_out,
    received,
    results,
    ga,
    gb,
    stage,
    acc,
    part,
    sums_dp,
    sums_mp,
    x_buf,
    l_buf,
    r_buf,
    o_buf,
    g_sem,
    stage_sem,
    block_sem,
    send_f,
    recv_f,
    send_r,
    recv_r,
    send_dp,
    recv_dp,
    send_mp,
    recv_mp,
):
    del packed_in
    peers, owned, rows, block = packed.shape
    matrices, _, width = g_ref.shape
    row_blocks = left_ref.shape[2]
    halves = block // rows
    me, mp = lax.axis_index("dp"), lax.axis_index("mp")
    my_block, my_half = me // halves, me % halves

    def peer(zo, ho):
        return peer_of(zo, ho, row_blocks, halves)

    barrier = pltpu.get_barrier_semaphore()
    for o in range(1, peers):
        q = (me + o) % peers
        pl.semaphore_signal(barrier, inc=1, device_id=(q, mp), device_id_type=MESH)
    for o in range(1, n_mp):
        q = (mp + o) % n_mp
        pl.semaphore_signal(barrier, inc=1, device_id=(me, q), device_id_type=MESH)
    pl.semaphore_wait(barrier, peers + n_mp - 2)

    def forward(q, j):
        return pltpu.make_async_remote_copy(
            src_ref=packed.at[q, j],
            dst_ref=received.at[me, j],
            send_sem=send_f.at[q, j],
            recv_sem=recv_f.at[me, j],
            device_id=(q, mp),
            device_id_type=MESH,
        )

    def arrival(q, j):
        return pltpu.make_async_remote_copy(
            src_ref=packed.at[q, j],
            dst_ref=received.at[q, j],
            send_sem=send_f.at[q, j],
            recv_sem=recv_f.at[q, j],
            device_id=(q, mp),
            device_id_type=MESH,
        )

    first = [(zo, ho) for zo in range(NEAR, row_blocks) for ho in range(halves)]
    later = [(zo, ho) for zo in range(1, NEAR) for ho in range(halves)]
    later = later + [(0, ho) for ho in range(1, halves)]
    for zo, ho in first:
        forward(peer(zo, ho), 0).start()

    chunk = ga.shape[1]
    cols = width // block
    chunks = rows // chunk
    rest = peers * owned - len(first)
    acc[...] = jnp.zeros_like(acc)

    def unit(n):
        n = n + len(first)
        k = n % peers
        return peer((k // halves + NEAR) % row_blocks, k % halves), n // peers

    def load(t):
        buf = ga if t % 2 == 0 else gb

        def column(i, _):
            at = pl.multiple_of((i % cols) * block, LANES)
            src = g_ref.at[i // cols, pl.ds(t * chunk, chunk), pl.ds(at, block)]
            pltpu.make_async_copy(src, buf.at[i], g_sem.at[t % 2]).start()
            return 0

        lax.fori_loop(0, matrices * cols, column, 0)

    def loaded(t):
        buf = ga if t % 2 == 0 else gb
        pltpu.make_async_copy(buf, buf, g_sem.at[t % 2]).wait()

    load(0)
    for t in range(chunks):
        g = ga if t % 2 == 0 else gb
        if t + 1 < chunks:
            load(t + 1)
        loaded(t)

        def stored(n, t=t):
            q, j = unit(n)
            return pltpu.make_async_copy(
                stage.at[n % RING],
                packed.at[q, j, pl.ds(t * chunk, chunk), :],
                stage_sem.at[n % RING],
            )

        def move(n, _, g=g, stored=stored):
            q, j = unit(n)

            @pl.when(n >= RING)
            def _():
                stored(n - RING).wait()

            stage[n % RING] = g[table_ref[q * owned + j]]
            stored(n).start()
            return 0

        def square(n, _, g=g):
            per = chunk // 16
            x = g[n // per, pl.ds(pl.multiple_of((n % per) * 16, 16), 16), :]
            wide = x.astype(jnp.float32)
            wide = wide * wide
            acc[...] += wide[:8] + wide[8:]
            return 0

        lax.fori_loop(0, rest, move, 0)
        lax.fori_loop(0, matrices * cols * (chunk // 16), square, 0)
        for n in range(max(rest - RING, 0), rest):
            stored(n).wait()

    for j in range(owned):
        for zo, ho in (first if j else []) + later:
            forward(peer(zo, ho), j).start()

    tile = acc[:, :LANES]
    for k in range(1, block // LANES):
        tile += acc[:, k * LANES : (k + 1) * LANES]
    part[0] = tile
    sums_dp[me] = tile

    def spread(o, axis_me, n, src, dst, send, recv, device):
        q = (axis_me + o) % n
        return pltpu.make_async_remote_copy(
            src_ref=src,
            dst_ref=dst.at[axis_me],
            send_sem=send.at[o],
            recv_sem=recv.at[axis_me],
            device_id=device(q),
            device_id_type=MESH,
        )

    def landed(o, axis_me, n, src, dst, send, recv, device):
        q = (axis_me + o) % n
        return pltpu.make_async_remote_copy(
            src_ref=src,
            dst_ref=dst.at[q],
            send_sem=send.at[o],
            recv_sem=recv.at[q],
            device_id=device(q),
            device_id_type=MESH,
        )

    dp_args = (me, peers, part.at[0], sums_dp, send_dp, recv_dp, lambda q: (q, mp))
    mp_args = (mp, n_mp, part.at[1], sums_mp, send_mp, recv_mp, lambda q: (me, q))
    for o in range(1, peers):
        spread(o, *dp_args).start()
    for o in range(1, peers):
        landed(o, *dp_args).wait_recv()
    tile = jnp.sum(sums_dp[...], axis=0)
    part[1] = tile
    sums_mp[mp] = tile
    for o in range(1, n_mp):
        spread(o, *mp_args).start()
    for o in range(1, n_mp):
        landed(o, *mp_args).wait_recv()
    tile = jnp.sum(sums_mp[...], axis=0)
    square_sum = jnp.sum(jnp.sum(tile, axis=0, keepdims=True), axis=1, keepdims=True)
    clip = jnp.minimum(1.0, rms_limit / jnp.sqrt(square_sum / total + epsilon))
    clip_out[0, 0] = clip[0, 0]
    for o in range(1, peers):
        spread(o, *dp_args).wait_send()
    for o in range(1, n_mp):
        spread(o, *mp_args).wait_send()

    def ret(q, j, r, h):
        return pltpu.make_async_remote_copy(
            src_ref=results.at[j, r, pl.ds(h * rows, rows), :],
            dst_ref=returned.at[me, j],
            send_sem=send_r.at[q, j],
            recv_sem=recv_r.at[me, j],
            device_id=(q, mp),
            device_id_type=MESH,
        )

    def home(q, j):
        return pltpu.make_async_remote_copy(
            src_ref=results.at[j, 0, pl.ds(0, rows), :],
            dst_ref=returned.at[q, j],
            send_sem=send_r.at[q, j],
            recv_sem=recv_r.at[q, j],
            device_id=(q, mp),
            device_id_type=MESH,
        )

    def one_block(n, _):
        j, k = n // row_blocks, n % row_blocks
        r = partner(my_block, (k + 1) % row_blocks, row_blocks)
        left = pltpu.make_async_copy(left_ref.at[j, 0, r], l_buf, block_sem.at[0])
        right = pltpu.make_async_copy(right_ref.at[j, 0, r], r_buf, block_sem.at[1])
        left.start()
        right.start()
        for h in range(halves):
            q = r * halves + h
            dst = x_buf.at[pl.ds(h * rows, rows), :]

            @pl.when(q == me)
            def _(q=q, h=h, dst=dst):
                pltpu.make_async_copy(packed.at[q, j], dst, block_sem.at[2 + h]).start()

            @pl.when(q != me)
            def _(q=q, h=h, dst=dst):
                arrival(q, j).wait_recv()
                pltpu.make_async_copy(received.at[q, j], dst, block_sem.at[2 + h]).start()

        left.wait()
        right.wait()
        for h in range(halves):
            dst = x_buf.at[pl.ds(h * rows, rows), :]
            pltpu.make_async_copy(packed.at[0, 0], dst, block_sem.at[2 + h]).wait()
        first = jnp.dot(l_buf[...], x_buf[...], preferred_element_type=jnp.float32)
        scaled = (clip_out[0, 0] * first).astype(jnp.bfloat16)
        second = jnp.dot(scaled, r_buf[...], preferred_element_type=jnp.float32)
        o_buf[...] = second.astype(o_buf.dtype)
        out = pltpu.make_async_copy(o_buf, results.at[j, r], block_sem.at[0])
        out.start()
        out.wait()
        for t in range(halves):
            h = partner(my_half, (t + mp) % halves, halves)
            q = r * halves + h

            @pl.when(q == me)
            def _(q=q, h=h):
                returned[me, j] = o_buf[pl.ds(pl.multiple_of(h * rows, 16), rows), :]

            @pl.when(q != me)
            def _(q=q, h=h):
                ret(q, j, r, h).start()

        return 0

    lax.fori_loop(0, owned * row_blocks, one_block, 0)

    for j in range(owned):
        for zo, ho in first + later:
            q = peer(zo, ho)
            forward(q, j).wait_send()
            home(q, j).wait_recv()
            home(q, j).wait_send()


def exchange(mesh, total, table, packed, gradients, left_roots, right_roots):
    peers, owned, rows, block = packed.shape
    matrices, _, width = gradients.shape
    row_blocks = left_roots.shape[2]
    n_mp = mesh.shape["mp"]
    chunk = max(c for c in range(16, 129, 16) if rows % c == 0)
    dtype = gradients.dtype
    dma = pltpu.SemaphoreType.DMA
    count = owned * row_blocks
    anywhere = pl.BlockSpec(memory_space=pltpu.HBM)
    in_vmem = pl.BlockSpec(memory_space=pltpu.VMEM)
    in_smem = pl.BlockSpec(memory_space=pltpu.SMEM)
    outs = pl.pallas_call(
        functools.partial(main_kernel, total, n_mp),
        in_specs=[pl.BlockSpec(memory_space=pltpu.SMEM)] + [anywhere] * 4,
        out_specs=[anywhere, in_vmem, in_smem, anywhere, anywhere],
        out_shape=[
            jax.ShapeDtypeStruct(packed.shape, dtype),
            pltpu.VMEM((peers, owned, rows, block), dtype),
            pltpu.SMEM((1, 1), jnp.float32),
            jax.ShapeDtypeStruct(packed.shape, dtype),
            jax.ShapeDtypeStruct((owned, row_blocks, block, block), dtype),
        ],
        scratch_shapes=[
            pltpu.VMEM((peers * owned, chunk, block), dtype),
            pltpu.VMEM((peers * owned, chunk, block), dtype),
            pltpu.VMEM((RING, chunk, block), dtype),
            pltpu.VMEM((8, block), jnp.float32),
            pltpu.VMEM((2, 8, LANES), jnp.float32),
            pltpu.VMEM((peers, 8, LANES), jnp.float32),
            pltpu.VMEM((n_mp, 8, LANES), jnp.float32),
            pltpu.VMEM((block, block), dtype),
            pltpu.VMEM((block, block), dtype),
            pltpu.VMEM((block, block), dtype),
            pltpu.VMEM((block, block), dtype),
            dma((2,)),
            dma((RING,)),
            dma((2 + block // rows,)),
            dma((peers, owned)),
            dma((peers, owned)),
            dma((peers, owned)),
            dma((peers, owned)),
            dma((peers,)),
            dma((peers,)),
            dma((n_mp,)),
            dma((n_mp,)),
        ],
        input_output_aliases={1: 0},
        compiler_params=pltpu.CompilerParams(
            collective_id=0, has_side_effects=True, vmem_limit_bytes=36 * MIB
        ),
        cost_estimate=pl.CostEstimate(
            flops=4 * count * block**3,
            bytes_accessed=8 * count * block**2,
            transcendentals=0,
        ),
    )(table, packed, gradients, left_roots, right_roots)
    return outs[1], outs[2]


def last_kernel(owned, table_ref, clip_ref, x_ref, o_ref, clip_out, sems):
    peers, _, rows, block = x_ref.shape
    cols = o_ref.shape[2] // block

    def put(s):
        m, c = table_ref[s] // cols, table_ref[s] % cols
        dst = o_ref.at[m, :, pl.ds(pl.multiple_of(c * block, LANES), block)]
        return pltpu.make_async_copy(x_ref.at[s // owned, s % owned], dst, sems.at[s])

    for s in range(peers * owned):
        put(s).start()
    clip_out[0, 0] = clip_ref[0, 0]
    for s in range(peers * owned):
        put(s).wait()


def unpack(table, clip, returned, shape):
    peers, owned, rows, block = returned.shape
    return pl.pallas_call(
        functools.partial(last_kernel, owned),
        in_specs=[
            pl.BlockSpec(memory_space=pltpu.SMEM),
            pl.BlockSpec(memory_space=pltpu.SMEM),
            pl.BlockSpec(memory_space=pltpu.VMEM),
        ],
        out_specs=[
            pl.BlockSpec(memory_space=pltpu.HBM),
            pl.BlockSpec(memory_space=pltpu.SMEM),
        ],
        out_shape=[
            jax.ShapeDtypeStruct(shape, returned.dtype),
            jax.ShapeDtypeStruct((1, 1), jnp.float32),
        ],
        scratch_shapes=[pltpu.SemaphoreType.DMA((peers * owned,))],
        compiler_params=pltpu.CompilerParams(vmem_limit_bytes=4 * MIB),
        cost_estimate=pl.CostEstimate(
            flops=0, bytes_accessed=2 * math.prod(shape), transcendentals=0
        ),
    )(table, clip, returned)


def body(mesh, total, gradients, column_slot, left_roots, right_roots):
    owned, block = left_roots.shape[0], left_roots.shape[-1]
    peers = mesh.shape["dp"]
    packed, table = first_pack(
        column_slot, gradients, peers, owned, left_roots.shape[2], block
    )
    returned, clip = exchange(
        mesh, total, table, packed, gradients, left_roots, right_roots
    )
    update, clip = unpack(table, clip, returned, gradients.shape)
    return (update, clip.reshape(()))


def solution(mesh):
    def run(gradients, column_slot, left_roots, right_roots):
        mapped = jax.shard_map(
            functools.partial(body, mesh, math.prod(gradients.shape)),
            mesh=mesh,
            in_specs=(
                P(None, "dp", "mp"),
                P(),
                P("dp", "mp", None, None, None),
                P("dp", "mp", None, None, None),
            ),
            out_specs=(P(None, "dp", "mp"), P()),
            check_vma=False,
        )
        return mapped(gradients, column_slot, left_roots, right_roots)

    return run
```

```python
import functools
import math

import jax
import jax.numpy as jnp
from jax import lax
from jax.experimental import pallas as pl
from jax.experimental.pallas import tpu as pltpu
from jax.sharding import PartitionSpec as P

rms_limit = 0.25
epsilon = 1e-06
MESH = pl.DeviceIdType.MESH
MIB = 1024 * 1024
LANES = 128
RING = 8


def partner(a, b, n):
    if n & (n - 1):
        return (a + b) % n
    total, bit = 0, 1
    while bit < n:
        total = total + ((a // bit + b // bit) % 2) * bit
        bit *= 2
    return total


def peer_of(zo, ho, row_blocks, halves):
    me, mp = lax.axis_index("dp"), lax.axis_index("mp")
    block, half = me // halves, me % halves
    if not (isinstance(zo, int) and zo == 0):
        ho = (ho + mp) % halves
    return partner(block, zo, row_blocks) * halves + partner(half, ho, halves)


NEAR = 2


def first_kernel(
    owned, row_blocks, slot_ref, g_ref, packed_ref, table_ref, buf, in_sem, out_sem
):
    matrices, rows, width = g_ref.shape
    block = packed_ref.shape[-1]
    peers = packed_ref.shape[0]
    halves = peers // row_blocks
    first = [
        peer_of(zo, ho, row_blocks, halves)
        for zo in range(NEAR, row_blocks)
        for ho in range(halves)
    ]
    cols = width // block
    base = lax.axis_index("mp") * cols
    for m in range(matrices):
        for c in range(cols):
            s = slot_ref[m, base + c]
            table_ref[s] = m * cols + c

    def read(k):
        s = table_ref[first[k] * owned]
        at = pl.multiple_of((s % cols) * block, LANES)
        src = g_ref.at[s // cols, :, pl.ds(at, block)]
        return pltpu.make_async_copy(src, buf.at[k], in_sem.at[k])

    def write(k):
        return pltpu.make_async_copy(buf.at[k], packed_ref.at[first[k], 0], out_sem.at[k])

    for k in range(len(first)):
        read(k).start()
    for k in range(len(first)):
        read(k).wait()
        write(k).start()
    for k in range(len(first)):
        write(k).wait()


def first_pack(column_slot, gradients, peers, owned, row_blocks, block):
    rows = gradients.shape[1]
    half = peers * rows * block
    return pl.pallas_call(
        functools.partial(first_kernel, owned, row_blocks),
        in_specs=[
            pl.BlockSpec(memory_space=pltpu.SMEM),
            pl.BlockSpec(memory_space=pltpu.HBM),
        ],
        out_specs=[
            pl.BlockSpec(memory_space=pltpu.HBM),
            pl.BlockSpec(memory_space=pltpu.SMEM),
        ],
        out_shape=[
            pltpu.HBM((peers, owned, rows, block), gradients.dtype),
            pltpu.SMEM((peers * owned,), jnp.int32),
        ],
        scratch_shapes=[
            pltpu.VMEM((peers, rows, block), gradients.dtype),
            pltpu.SemaphoreType.DMA((peers,)),
            pltpu.SemaphoreType.DMA((peers,)),
        ],
        compiler_params=pltpu.CompilerParams(vmem_limit_bytes=56 * MIB),
        cost_estimate=pl.CostEstimate(flops=0, bytes_accessed=4 * half, transcendentals=0),
    )(column_slot, gradients)


def main_kernel(
    total,
    n_mp,
    table_ref,
    packed_in,
    g_ref,
    left_ref,
    right_ref,
    packed,
    returned,
    clip_out,
    received,
    results,
    ga,
    gb,
    stage,
    acc,
    part,
    sums_dp,
    sums_mp,
    x_buf,
    l_buf,
    r_buf,
    o_buf,
    g_sem,
    stage_sem,
    block_sem,
    send_f,
    recv_f,
    send_r,
    recv_r,
    send_dp,
    recv_dp,
    send_mp,
    recv_mp,
):
    del packed_in
    peers, owned, rows, block = packed.shape
    matrices, _, width = g_ref.shape
    row_blocks = left_ref.shape[2]
    halves = block // rows
    me, mp = lax.axis_index("dp"), lax.axis_index("mp")
    my_block, my_half = me // halves, me % halves

    def peer(zo, ho):
        return peer_of(zo, ho, row_blocks, halves)

    barrier = pltpu.get_barrier_semaphore()
    for o in range(1, peers):
        q = (me + o) % peers
        pl.semaphore_signal(barrier, inc=1, device_id=(q, mp), device_id_type=MESH)
    for o in range(1, n_mp):
        q = (mp + o) % n_mp
        pl.semaphore_signal(barrier, inc=1, device_id=(me, q), device_id_type=MESH)
    pl.semaphore_wait(barrier, peers + n_mp - 2)

    def forward(q, j):
        return pltpu.make_async_remote_copy(
            src_ref=packed.at[q, j],
            dst_ref=received.at[me, j],
            send_sem=send_f.at[q, j],
            recv_sem=recv_f.at[me, j],
            device_id=(q, mp),
            device_id_type=MESH,
        )

    def arrival(q, j):
        return pltpu.make_async_remote_copy(
            src_ref=packed.at[q, j],
            dst_ref=received.at[q, j],
            send_sem=send_f.at[q, j],
            recv_sem=recv_f.at[q, j],
            device_id=(q, mp),
            device_id_type=MESH,
        )

    first = [(zo, ho) for zo in range(NEAR, row_blocks) for ho in range(halves)]
    later = [(zo, ho) for zo in range(1, NEAR) for ho in range(halves)]
    later = later + [(0, ho) for ho in range(1, halves)]
    for zo, ho in first:
        forward(peer(zo, ho), 0).start()

    chunk = ga.shape[1]
    cols = width // block
    chunks = rows // chunk
    rest = peers * owned - len(first)

    def unit(n):
        n = n + len(first)
        k = n % peers
        return peer((k // halves + NEAR) % row_blocks, k % halves), n // peers

    def load(t):
        buf = ga if t % 2 == 0 else gb

        def column(i, _):
            at = pl.multiple_of((i % cols) * block, LANES)
            src = g_ref.at[i // cols, pl.ds(t * chunk, chunk), pl.ds(at, block)]
            pltpu.make_async_copy(src, buf.at[i], load_sem).start()
            return 0

        load_sem = g_sem.at[0] if buf is ga else g_sem.at[1]
        lax.fori_loop(0, matrices * cols, column, 0)

    def loaded(t):
        buf = ga if t % 2 == 0 else gb
        pltpu.make_async_copy(buf, buf, g_sem.at[t % 2]).wait()
        return buf

    acc[...] = jnp.zeros_like(acc)
    load(0)
    for t in range(chunks):
        if t + 1 < chunks:
            load(t + 1)
        g = loaded(t)

        def stored(n, t=t):
            q, j = unit(n)
            return pltpu.make_async_copy(
                stage.at[n % RING],
                packed.at[q, j, pl.ds(t * chunk, chunk), :],
                stage_sem.at[n % RING],
            )

        def move(n, _, g=g, stored=stored):
            q, j = unit(n)

            @pl.when(n >= RING)
            def _():
                stored(n - RING).wait()

            stage[n % RING] = g[table_ref[q * owned + j]]
            stored(n).start()
            return 0

        def square(n, _, g=g):
            wide = g[n].astype(jnp.float32)
            acc[...] += jnp.sum((wide * wide).reshape(-1, 8, block), axis=0)
            return 0

        lax.fori_loop(0, rest, move, 0)
        lax.fori_loop(0, matrices * cols, square, 0)
        for n in range(max(rest - RING, 0), rest):
            stored(n).wait()

    tile = acc[:, :LANES]
    for k in range(1, block // LANES):
        tile += acc[:, k * LANES : (k + 1) * LANES]
    part[0] = tile
    sums_dp[me] = tile

    def spread(o, axis_me, n, src, dst, send, recv, device):
        q = (axis_me + o) % n
        return pltpu.make_async_remote_copy(
            src_ref=src,
            dst_ref=dst.at[axis_me],
            send_sem=send.at[o],
            recv_sem=recv.at[axis_me],
            device_id=device(q),
            device_id_type=MESH,
        )

    def landed(o, axis_me, n, src, dst, send, recv, device):
        q = (axis_me + o) % n
        return pltpu.make_async_remote_copy(
            src_ref=src,
            dst_ref=dst.at[q],
            send_sem=send.at[o],
            recv_sem=recv.at[q],
            device_id=device(q),
            device_id_type=MESH,
        )

    dp_args = (me, peers, part.at[0], sums_dp, send_dp, recv_dp, lambda q: (q, mp))
    mp_args = (mp, n_mp, part.at[1], sums_mp, send_mp, recv_mp, lambda q: (me, q))
    for o in range(1, peers):
        spread(o, *dp_args).start()
    for j in range(owned):
        for zo, ho in (first if j else []) + later:
            forward(peer(zo, ho), j).start()
    for o in range(1, peers):
        landed(o, *dp_args).wait_recv()
    tile = jnp.sum(sums_dp[...], axis=0)
    part[1] = tile
    sums_mp[mp] = tile
    for o in range(1, n_mp):
        spread(o, *mp_args).start()
    for o in range(1, n_mp):
        landed(o, *mp_args).wait_recv()
    tile = jnp.sum(sums_mp[...], axis=0)
    square_sum = jnp.sum(jnp.sum(tile, axis=0, keepdims=True), axis=1, keepdims=True)
    clip = jnp.minimum(1.0, rms_limit / jnp.sqrt(square_sum / total + epsilon))
    clip_out[0, 0] = clip[0, 0]
    for o in range(1, peers):
        spread(o, *dp_args).wait_send()
    for o in range(1, n_mp):
        spread(o, *mp_args).wait_send()

    def ret(q, j, r, h):
        return pltpu.make_async_remote_copy(
            src_ref=results.at[j, r, pl.ds(h * rows, rows), :],
            dst_ref=returned.at[me, j],
            send_sem=send_r.at[q, j],
            recv_sem=recv_r.at[me, j],
            device_id=(q, mp),
            device_id_type=MESH,
        )

    def home(q, j):
        return pltpu.make_async_remote_copy(
            src_ref=results.at[j, 0, pl.ds(0, rows), :],
            dst_ref=returned.at[q, j],
            send_sem=send_r.at[q, j],
            recv_sem=recv_r.at[q, j],
            device_id=(q, mp),
            device_id_type=MESH,
        )

    def one_block(n, _):
        j, k = n // row_blocks, n % row_blocks
        r = partner(my_block, (k + 1) % row_blocks, row_blocks)
        left = pltpu.make_async_copy(left_ref.at[j, 0, r], l_buf, block_sem.at[0])
        right = pltpu.make_async_copy(right_ref.at[j, 0, r], r_buf, block_sem.at[1])
        left.start()
        right.start()
        for h in range(halves):
            q = r * halves + h
            dst = x_buf.at[pl.ds(h * rows, rows), :]

            @pl.when(q == me)
            def _(q=q, h=h, dst=dst):
                pltpu.make_async_copy(packed.at[q, j], dst, block_sem.at[2 + h]).start()

            @pl.when(q != me)
            def _(q=q, h=h, dst=dst):
                arrival(q, j).wait_recv()
                pltpu.make_async_copy(received.at[q, j], dst, block_sem.at[2 + h]).start()

        left.wait()
        right.wait()
        for h in range(halves):
            dst = x_buf.at[pl.ds(h * rows, rows), :]
            pltpu.make_async_copy(packed.at[0, 0], dst, block_sem.at[2 + h]).wait()
        first = jnp.dot(l_buf[...], x_buf[...], preferred_element_type=jnp.float32)
        scaled = (clip_out[0, 0] * first).astype(jnp.bfloat16)
        second = jnp.dot(scaled, r_buf[...], preferred_element_type=jnp.float32)
        o_buf[...] = second.astype(o_buf.dtype)
        out = pltpu.make_async_copy(o_buf, results.at[j, r], block_sem.at[0])
        out.start()
        out.wait()
        for t in range(halves):
            h = partner(my_half, (t + mp) % halves, halves)
            q = r * halves + h

            @pl.when(q == me)
            def _(q=q, h=h):
                returned[me, j] = o_buf[pl.ds(pl.multiple_of(h * rows, 16), rows), :]

            @pl.when(q != me)
            def _(q=q, h=h):
                ret(q, j, r, h).start()

        return 0

    lax.fori_loop(0, owned * row_blocks, one_block, 0)

    for j in range(owned):
        for zo, ho in first + later:
            q = peer(zo, ho)
            forward(q, j).wait_send()
            home(q, j).wait_recv()
            home(q, j).wait_send()


def exchange(mesh, total, table, packed, gradients, left_roots, right_roots):
    peers, owned, rows, block = packed.shape
    matrices, _, width = gradients.shape
    row_blocks = left_roots.shape[2]
    n_mp = mesh.shape["mp"]
    chunk = max(c for c in range(16, 129, 16) if rows % c == 0)
    dtype = gradients.dtype
    dma = pltpu.SemaphoreType.DMA
    count = owned * row_blocks
    anywhere = pl.BlockSpec(memory_space=pltpu.HBM)
    in_vmem = pl.BlockSpec(memory_space=pltpu.VMEM)
    in_smem = pl.BlockSpec(memory_space=pltpu.SMEM)
    outs = pl.pallas_call(
        functools.partial(main_kernel, total, n_mp),
        in_specs=[pl.BlockSpec(memory_space=pltpu.SMEM)] + [anywhere] * 4,
        out_specs=[anywhere, in_vmem, in_smem, anywhere, anywhere],
        out_shape=[
            jax.ShapeDtypeStruct(packed.shape, dtype),
            pltpu.VMEM((peers, owned, rows, block), dtype),
            pltpu.SMEM((1, 1), jnp.float32),
            jax.ShapeDtypeStruct(packed.shape, dtype),
            jax.ShapeDtypeStruct((owned, row_blocks, block, block), dtype),
        ],
        scratch_shapes=[
            pltpu.VMEM((peers * owned, chunk, block), dtype),
            pltpu.VMEM((peers * owned, chunk, block), dtype),
            pltpu.VMEM((RING, chunk, block), dtype),
            pltpu.VMEM((8, block), jnp.float32),
            pltpu.VMEM((2, 8, LANES), jnp.float32),
            pltpu.VMEM((peers, 8, LANES), jnp.float32),
            pltpu.VMEM((n_mp, 8, LANES), jnp.float32),
            pltpu.VMEM((block, block), dtype),
            pltpu.VMEM((block, block), dtype),
            pltpu.VMEM((block, block), dtype),
            pltpu.VMEM((block, block), dtype),
            dma((2,)),
            dma((RING,)),
            dma((2 + block // rows,)),
            dma((peers, owned)),
            dma((peers, owned)),
            dma((peers, owned)),
            dma((peers, owned)),
            dma((peers,)),
            dma((peers,)),
            dma((n_mp,)),
            dma((n_mp,)),
        ],
        input_output_aliases={1: 0},
        compiler_params=pltpu.CompilerParams(
            collective_id=0, has_side_effects=True, vmem_limit_bytes=36 * MIB
        ),
        cost_estimate=pl.CostEstimate(
            flops=4 * count * block**3,
            bytes_accessed=8 * count * block**2,
            transcendentals=0,
        ),
    )(table, packed, gradients, left_roots, right_roots)
    return outs[1], outs[2]


def last_kernel(owned, table_ref, clip_ref, x_ref, o_ref, clip_out, sems):
    peers, _, rows, block = x_ref.shape
    cols = o_ref.shape[2] // block

    def put(s):
        m, c = table_ref[s] // cols, table_ref[s] % cols
        dst = o_ref.at[m, :, pl.ds(pl.multiple_of(c * block, LANES), block)]
        return pltpu.make_async_copy(x_ref.at[s // owned, s % owned], dst, sems.at[s])

    for s in range(peers * owned):
        put(s).start()
    clip_out[0, 0] = clip_ref[0, 0]
    for s in range(peers * owned):
        put(s).wait()


def unpack(table, clip, returned, shape):
    peers, owned, rows, block = returned.shape
    return pl.pallas_call(
        functools.partial(last_kernel, owned),
        in_specs=[
            pl.BlockSpec(memory_space=pltpu.SMEM),
            pl.BlockSpec(memory_space=pltpu.SMEM),
            pl.BlockSpec(memory_space=pltpu.VMEM),
        ],
        out_specs=[
            pl.BlockSpec(memory_space=pltpu.HBM),
            pl.BlockSpec(memory_space=pltpu.SMEM),
        ],
        out_shape=[
            jax.ShapeDtypeStruct(shape, returned.dtype),
            jax.ShapeDtypeStruct((1, 1), jnp.float32),
        ],
        scratch_shapes=[pltpu.SemaphoreType.DMA((peers * owned,))],
        compiler_params=pltpu.CompilerParams(vmem_limit_bytes=4 * MIB),
        cost_estimate=pl.CostEstimate(
            flops=0, bytes_accessed=2 * math.prod(shape), transcendentals=0
        ),
    )(table, clip, returned)


def body(mesh, total, gradients, column_slot, left_roots, right_roots):
    owned, block = left_roots.shape[0], left_roots.shape[-1]
    peers = mesh.shape["dp"]
    packed, table = first_pack(
        column_slot, gradients, peers, owned, left_roots.shape[2], block
    )
    returned, clip = exchange(
        mesh, total, table, packed, gradients, left_roots, right_roots
    )
    update, clip = unpack(table, clip, returned, gradients.shape)
    return (update, clip.reshape(()))


def solution(mesh):
    def run(gradients, column_slot, left_roots, right_roots):
        mapped = jax.shard_map(
            functools.partial(body, mesh, math.prod(gradients.shape)),
            mesh=mesh,
            in_specs=(
                P(None, "dp", "mp"),
                P(),
                P("dp", "mp", None, None, None),
                P("dp", "mp", None, None, None),
            ),
            out_specs=(P(None, "dp", "mp"), P()),
            check_vma=False,
        )
        return mapped(gradients, column_slot, left_roots, right_roots)

    return run
```
